128 devices in a mesh: data: 1, spatial: 64 (over z, y, x), model: 2 (over core).
Axes of the slice: x: 4, y: 4, z: 4, core: 2. Of those that a mesh axis runs over, the one named last changes fastest.
Arguments:
- images: bfloat16 [32, 1024, 14, 512], P('data', 'spatial')
- w_conv1: bfloat16 [3, 3, 512, 512], P(None, None, None, 'model')
- b_conv1: float32 [512], P('model')
- w_conv2: bfloat16 [3, 3, 512, 512], P(None, None, 'model')
- b_conv2: float32 [512], replicated
- w_conv3: bfloat16 [3, 3, 512, 512], P(None, None, None, 'model')
- b_conv3: float32 [512], P('model')
Outputs:
- output: bfloat16 [32, 1024, 14, 512], P('data', 'spatial', None, 'model')
All inputs are finite; a program needn't handle non-finite values.
Results may differ from the reference program's by a relative error of at most 0.00182.
Values are sent between devices in bfloat16 or wider.
A program may use at most 1 GiB of HBM per device.

```python
import jax
import jax.numpy as jnp
from jax import lax

IMG_BATCH = 32
IMG_HEIGHT = 1024
IMG_WIDTH = 14
CH_IN = 512
CH_ONE = 512
CH_TWO = 512
CH_OUT = 512


def setup_inputs(seed: int = 0, part: int = 0) -> dict:
    keys = jax.random.split(jax.random.key(seed), 7)
    img_key = jax.random.fold_in(keys[0], part)
    images = jax.random.normal(img_key, (IMG_BATCH, IMG_HEIGHT, IMG_WIDTH, CH_IN), jnp.float32)
    w_conv1 = jax.random.normal(keys[1], (3, 3, CH_IN, CH_ONE), jnp.float32) * (2.0 / (9 * CH_IN)) ** 0.5
    b_conv1 = 0.3 * jax.random.normal(keys[2], (CH_ONE,), jnp.float32)
    w_conv2 = jax.random.normal(keys[3], (3, 3, CH_ONE, CH_TWO), jnp.float32) * (2.0 / (9 * CH_ONE)) ** 0.5
    b_conv2 = 0.3 * jax.random.normal(keys[4], (CH_TWO,), jnp.float32)
    w_conv3 = jax.random.normal(keys[5], (3, 3, CH_TWO, CH_OUT), jnp.float32) * (2.0 / (9 * CH_TWO)) ** 0.5
    b_conv3 = 0.3 * jax.random.normal(keys[6], (CH_OUT,), jnp.float32)
    return {
        "images": images.astype(jnp.bfloat16),
        "w_conv1": w_conv1.astype(jnp.bfloat16),
        "b_conv1": b_conv1,
        "w_conv2": w_conv2.astype(jnp.bfloat16),
        "b_conv2": b_conv2,
        "w_conv3": w_conv3.astype(jnp.bfloat16),
        "b_conv3": b_conv3,
    }


def conv_same(feature, kernel):
    return lax.conv_general_dilated(feature[None], kernel, (1, 1), "SAME", dimension_numbers=("NHWC", "HWIO", "NHWC"))[0]


def reference(images, w_conv1, b_conv1, w_conv2, b_conv2, w_conv3, b_conv3):
    kern_one = w_conv1.astype(jnp.float32)
    kern_two = w_conv2.astype(jnp.float32)
    kern_three = w_conv3.astype(jnp.float32)

    def one_picture(picture):
        act_one = jax.nn.relu(conv_same(picture.astype(jnp.float32), kern_one) + b_conv1).astype(jnp.bfloat16)
        act_two = jax.nn.relu(conv_same(act_one.astype(jnp.float32), kern_two) + b_conv2).astype(jnp.bfloat16)
        return jax.nn.relu(conv_same(act_two.astype(jnp.float32), kern_three) + b_conv3).astype(jnp.bfloat16)

    return lax.map(one_picture, images)
```

```python
import functools

import jax
import jax.numpy as jnp
from jax import lax
from jax.experimental import pallas as pl
from jax.experimental.pallas import tpu as pltpu
from jax.sharding import PartitionSpec as P

MESH = pl.DeviceIdType.MESH
ROWS = 4


def kernel(
    dims, img, w1, b1, w2, b2, w3, b3, out,
    stage, act, wts, bias_own, bias_far,
    img_sem, w_sem, w_send, w_recv, b_sem, b_send, b_recv, h_send, h_recv, o_sem, o_send, o_recv,
):
    n_band, batch, height, width, ch = dims
    half, per_core = ch // 2, batch // 2
    core = lax.axis_index("model")
    band = lax.axis_index("spatial")
    data = lax.axis_index("data")
    above, below = lax.rem(band + n_band - 1, n_band), lax.rem(band + 1, n_band)
    sibling = (data, band, 1 - core)
    top, bottom = height + 2, height + 3

    to_above = jnp.where(band == 0, bottom, height + 1)
    to_below = jnp.where(band == n_band - 1, top, 0)

    images_in = pltpu.make_async_copy(img.at[pl.ds(core * per_core, per_core)], stage, img_sem)
    images_in.start()
    own_parts = [wts.at[0, :, :, 0:half], wts.at[1, :, 0:half, :], wts.at[2, :, :, 0:half]]
    far_parts = [wts.at[0, :, :, half:ch], wts.at[1, :, half:ch, :], wts.at[2, :, :, half:ch]]
    w_in = [pltpu.make_async_copy(w, own_parts[i], w_sem.at[i]) for i, w in enumerate((w1, w2, w3))]
    b_in = [
        pltpu.make_async_copy(b1, bias_own.at[0], b_sem.at[0]),
        pltpu.make_async_copy(b2.at[:, 0:half], bias_own.at[1], b_sem.at[1]),
        pltpu.make_async_copy(b2.at[:, half:ch], bias_far.at[1], b_sem.at[2]),
        pltpu.make_async_copy(b3, bias_own.at[2], b_sem.at[3]),
    ]
    w_in[0].start()
    for c in b_in:
        c.start()

    zero_row = jnp.zeros((width + 2, per_core, ch), jnp.bfloat16)
    zero_col = jnp.zeros((1, per_core, ch), jnp.bfloat16)

    def zero(level, _):
        act[level, 0] = zero_row
        act[level, height + 1] = zero_row

        def cols(r, _):
            act[level, r, 0:1] = zero_col
            act[level, r, width + 1 : width + 2] = zero_col
            return 0

        lax.fori_loop(1, height + 1, cols, 0)
        return 0

    lax.fori_loop(0, 3, zero, 0)

    barrier = pltpu.get_barrier_semaphore()
    for who in ((data, above, core), (data, below, core), sibling):
        pl.semaphore_signal(barrier, inc=1, device_id=who, device_id_type=MESH)
    pl.semaphore_wait(barrier, 3)

    w_far = [
        pltpu.make_async_remote_copy(w, far_parts[i], w_send.at[i], w_recv.at[i], device_id=sibling, device_id_type=MESH)
        for i, w in enumerate((w1, w2, w3))
    ]
    b_far = [
        pltpu.make_async_remote_copy(b, bias_far.at[i], b_send.at[k], b_recv.at[k], device_id=sibling, device_id_type=MESH)
        for k, (b, i) in enumerate(((b1, 0), (b3, 2)))
    ]
    w_far[0].start()
    for c in b_far:
        c.start()

    def halo_up(level):
        return pltpu.make_async_remote_copy(
            act.at[level, 1, 1 : width + 1], act.at[level, to_above, 1 : width + 1],
            h_send.at[level, 0], h_recv.at[level, 0], device_id=(data, above, core), device_id_type=MESH,
        )

    def halo_down(level):
        return pltpu.make_async_remote_copy(
            act.at[level, height, 1 : width + 1], act.at[level, to_below, 1 : width + 1],
            h_send.at[level, 1], h_recv.at[level, 1], device_id=(data, below, core), device_id_type=MESH,
        )

    def send_halo(level):
        halo_up(level).start()
        halo_down(level).start()

    def wait_halo(level):
        halo_up(level).wait_recv()
        halo_down(level).wait_recv()

    def take(col, _):
        act[0, 1 : height + 1, col + 1] = jnp.swapaxes(stage[:, col], 0, 1)
        return 0

    images_in.wait()
    lax.fori_loop(0, width, take, 0)
    send_halo(0)
    w_in[1].start()
    w_in[2].start()
    w_far[1].start()
    w_far[2].start()
    for c in b_in:
        c.wait()
    for c in b_far:
        c.wait_recv()

    def conv(level, rows):
        m = width * per_core
        taps = []
        for dh in range(3):
            for dw in range(3):
                views = [act[level, r + dh, dw : dw + width].reshape(m, ch) for r in rows]
                taps.append(jnp.concatenate(views, axis=0))
        lhs = jnp.concatenate(taps, axis=1)
        total = jnp.dot(lhs, wts[level].reshape(9 * ch, ch), preferred_element_type=jnp.float32)
        bias = jnp.concatenate([bias_own[level], bias_far[level]], axis=1)
        return jnp.maximum(total + bias, 0.0).astype(jnp.bfloat16).reshape(ROWS, width, per_core, ch)

    n_chunk = height // ROWS

    def rows_of(j):
        return [lax.rem(1 + ROWS * j + i, height) for i in range(ROWS)]

    def layer(level):
        w_in[level].wait()
        w_far[level].wait_recv()

        def chunk(j, _):
            @pl.when(j == n_chunk - 1)
            def _():
                wait_halo(level)

            rows = rows_of(j)
            y = conv(level, rows)
            for i, r in enumerate(rows):
                act[(level + 1) % 3, r + 1, 1 : width + 1] = y[i]
            return 0

        lax.fori_loop(0, n_chunk, chunk, 0)

    layer(0)
    send_halo(1)
    layer(1)
    send_halo(2)
    halo_up(0).wait_send()
    halo_down(0).wait_send()
    layer(2)

    mine = pl.ds(core * per_core, per_core)

    def own_out(col):
        return pltpu.make_async_copy(stage.at[:, col, :, 0:half], out.at[mine, col], o_sem.at[col])

    def far_out(col):
        return pltpu.make_async_remote_copy(
            stage.at[:, col, :, half:ch], out.at[mine, col], o_send.at[col], o_recv.at[col],
            device_id=sibling, device_id_type=MESH,
        )

    def give(col, _):
        stage[:, col] = jnp.swapaxes(act[0, 1 : height + 1, col + 1], 0, 1)
        far_out(col).start()
        own_out(col).start()
        return 0

    lax.fori_loop(0, width, give, 0)

    for i in range(3):
        w_far[i].wait_send()
    for level in (1, 2):
        halo_up(level).wait_send()
        halo_down(level).wait_send()
    for c in b_far:
        c.wait_send()

    def finish(col, _):
        own_out(col).wait()
        far_out(col).wait_send()
        far_out(col).wait_recv()
        return 0

    lax.fori_loop(0, width, finish, 0)


def solution(mesh):
    n_band = mesh.shape["spatial"]

    def local_stack(images, w_conv1, b_conv1, w_conv2, b_conv2, w_conv3, b_conv3):
        batch, height, width, ch = images.shape
        half, per_core = ch // 2, batch // 2
        hbm = pl.BlockSpec(memory_space=pltpu.HBM)
        dma = pltpu.SemaphoreType.DMA
        flops = 2 * 3 * 9 * per_core * height * width * ch * ch
        y = pl.pallas_call(
            functools.partial(kernel, (n_band, batch, height, width, ch)),
            out_shape=jax.ShapeDtypeStruct((batch, width, height, half), jnp.bfloat16),
            in_specs=[hbm] * 7,
            out_specs=hbm,
            scratch_shapes=[
                pltpu.VMEM((per_core, width, height, ch), jnp.bfloat16),
                pltpu.VMEM((3, height + 4, width + 2, per_core, ch), jnp.bfloat16),
                pltpu.VMEM((3, 9, ch, ch), jnp.bfloat16),
                pltpu.VMEM((3, 1, half), jnp.float32),
                pltpu.VMEM((3, 1, half), jnp.float32),
                dma,
                dma((3,)), dma((3,)), dma((3,)),
                dma((4,)), dma((2,)), dma((2,)),
                dma((3, 2)), dma((3, 2)),
                dma((width,)), dma((width,)), dma((width,)),
            ],
            compiler_params=pltpu.CompilerParams(
                collective_id=0, has_side_effects=True, vmem_limit_bytes=62 * 1024 * 1024
            ),
            cost_estimate=pl.CostEstimate(flops=flops, bytes_accessed=40_000_000, transcendentals=0),
        )(
            jnp.swapaxes(images, 1, 2),
            w_conv1.reshape(9, ch, half), b_conv1.reshape(1, half),
            w_conv2.reshape(9, half, ch), b_conv2.reshape(1, ch),
            w_conv3.reshape(9, ch, half), b_conv3.reshape(1, half),
        )
        return jnp.swapaxes(y, 1, 2)

    in_specs = (
        P("data", "spatial", None, None),
        P(None, None, None, "model"),
        P("model"),
        P(None, None, "model", None),
        P(None),
        P(None, None, None, "model"),
        P("model"),
    )
    return jax.shard_map(local_stack, mesh=mesh, in_specs=in_specs, out_specs=P("data", "spatial", None, "model"), check_vma=False)
```

```python
import functools

import jax
import jax.numpy as jnp
from jax import lax
from jax.experimental import pallas as pl
from jax.experimental.pallas import tpu as pltpu
from jax.sharding import PartitionSpec as P

MESH = pl.DeviceIdType.MESH
ROWS = 4
VMEM_LIMIT = 48 * 1024 * 1024


def convs(
    dims, img, w1, b1, w2, b2, w3, b3, own, far,
    stage, act, wts, bias_own, bias_far,
    img_sem, w_sem, w_send, w_recv, b_sem, b_send, b_recv, h_send, h_recv, o_send, o_recv,
):
    n_band, per_core, height, width, ch = dims
    half = ch // 2
    core = lax.axis_index("model")
    band = lax.axis_index("spatial")
    data = lax.axis_index("data")
    first, final = band == 0, band == n_band - 1
    above, below = jnp.maximum(band - 1, 0), jnp.minimum(band + 1, n_band - 1)
    sibling = (data, band, 1 - core)

    def image_in(col):
        return pltpu.make_async_copy(img.at[pl.ds(core * per_core, per_core), col], stage.at[:, col], img_sem.at[col])

    own_parts = [wts.at[0, :, :, 0:half], wts.at[1, :, 0:half, :], wts.at[2, :, :, 0:half]]
    far_parts = [wts.at[0, :, :, half:ch], wts.at[1, :, half:ch, :], wts.at[2, :, :, half:ch]]
    w_in = [pltpu.make_async_copy(w, own_parts[i], w_sem.at[i]) for i, w in enumerate((w1, w2, w3))]
    w_far = [
        pltpu.make_async_remote_copy(w, far_parts[i], w_send.at[i], w_recv.at[i], device_id=sibling, device_id_type=MESH)
        for i, w in enumerate((w1, w2, w3))
    ]
    b_in = [
        pltpu.make_async_copy(b1, bias_own.at[0], b_sem.at[0]),
        pltpu.make_async_copy(b2.at[:, 0:half], bias_own.at[1], b_sem.at[1]),
        pltpu.make_async_copy(b2.at[:, half:ch], bias_far.at[1], b_sem.at[2]),
        pltpu.make_async_copy(b3, bias_own.at[2], b_sem.at[3]),
    ]
    b_far = [
        pltpu.make_async_remote_copy(b, bias_far.at[i], b_send.at[k], b_recv.at[k], device_id=sibling, device_id_type=MESH)
        for k, (b, i) in enumerate(((b1, 0), (b3, 2)))
    ]

    barrier = pltpu.get_barrier_semaphore()
    pl.semaphore_signal(barrier, inc=1, device_id=sibling, device_id_type=MESH)

    @pl.when(jnp.logical_not(first))
    def _():
        pl.semaphore_signal(barrier, inc=1, device_id=(data, above, core), device_id_type=MESH)

    @pl.when(jnp.logical_not(final))
    def _():
        pl.semaphore_signal(barrier, inc=1, device_id=(data, below, core), device_id_type=MESH)

    for col in range(width):
        image_in(col).start()
    w_in[0].start()
    for c in b_in:
        c.start()
    pl.semaphore_wait(barrier, 3 - first.astype(jnp.int32) - final.astype(jnp.int32))
    w_far[0].start()
    for c in b_far:
        c.start()

    zero_row = jnp.zeros((width, per_core, ch), jnp.bfloat16)
    zero_col = jnp.zeros((1, per_core, ch), jnp.bfloat16)

    def zero(level, _):
        def cols(r, _):
            act[level, r, 0:1] = zero_col
            act[level, r, width + 1 : width + 2] = zero_col
            return 0

        lax.fori_loop(0, height + 2, cols, 0)

        @pl.when(first)
        def _():
            act[level, 0, 1 : width + 1] = zero_row

        @pl.when(final)
        def _():
            act[level, height + 1, 1 : width + 1] = zero_row

        return 0

    lax.fori_loop(0, 3, zero, 0)

    def halo_up(level):
        return pltpu.make_async_remote_copy(
            act.at[level, 1, 1 : width + 1], act.at[level, height + 1, 1 : width + 1],
            h_send.at[level, 0], h_recv.at[level, 0], device_id=(data, above, core), device_id_type=MESH,
        )

    def halo_down(level):
        return pltpu.make_async_remote_copy(
            act.at[level, height, 1 : width + 1], act.at[level, 0, 1 : width + 1],
            h_send.at[level, 1], h_recv.at[level, 1], device_id=(data, below, core), device_id_type=MESH,
        )

    def send_halo(level):
        @pl.when(jnp.logical_not(first))
        def _():
            halo_up(level).start()

        @pl.when(jnp.logical_not(final))
        def _():
            halo_down(level).start()

    def wait_halo(level):
        @pl.when(jnp.logical_not(final))
        def _():
            halo_up(level).wait_recv()

        @pl.when(jnp.logical_not(first))
        def _():
            halo_down(level).wait_recv()

    def sent_halo(level):
        @pl.when(jnp.logical_not(first))
        def _():
            halo_up(level).wait_send()

        @pl.when(jnp.logical_not(final))
        def _():
            halo_down(level).wait_send()

    def take(col, _):
        image_in(col).wait()
        act[0, 1 : height + 1, col + 1] = jnp.swapaxes(stage[:, col], 0, 1)
        return 0

    lax.fori_loop(0, width, take, 0)
    send_halo(0)
    w_in[1].start()
    w_in[2].start()
    w_far[1].start()
    w_far[2].start()

    def conv(level, rows, lo, hi):
        m = width * per_core
        taps = []
        for dh in range(3):
            for dw in range(3):
                views = [act[level, r + dh, dw : dw + width].reshape(m, ch) for r in rows]
                taps.append(jnp.concatenate(views, axis=0))
        lhs = jnp.concatenate(taps, axis=1)
        total = jnp.dot(lhs, wts[level, :, :, lo:hi].reshape(9 * ch, hi - lo), preferred_element_type=jnp.float32)
        bias = ([bias_own[level]] if lo == 0 else []) + ([bias_far[level]] if hi == ch else [])
        total = total + (jnp.concatenate(bias, axis=1) if len(bias) > 1 else bias[0])
        return jnp.maximum(total, 0.0).astype(jnp.bfloat16).reshape(len(rows), width, per_core, hi - lo)

    def step(level, rows, lo=0, hi=ch):
        y = conv(level, rows, lo, hi)
        for i, r in enumerate(rows):
            act[level + 1, r + 1, 1 : width + 1, :, lo:hi] = y[i]

    inner = [list(range(r, min(r + ROWS, height - 1))) for r in range(1, height - 1, ROWS)]
    outer = [height - 1, 0]

    w_in[0].wait()
    for c in b_in:
        c.wait()
    for rows in inner[:2]:
        step(0, rows, 0, half)
    w_far[0].wait_recv()
    for c in b_far:
        c.wait_recv()
    for rows in inner[:2]:
        step(0, rows, half, ch)
    for rows in inner[2:]:
        step(0, rows)
    wait_halo(0)
    step(0, outer)
    send_halo(1)

    w_in[1].wait()
    w_far[1].wait_recv()
    for rows in inner:
        step(1, rows)
    wait_halo(1)
    step(1, outer)
    send_halo(2)

    def to_sibling(r):
        return pltpu.make_async_remote_copy(
            act.at[0, r + 1, 1 : width + 1, :, half:ch], far.at[r], o_send.at[r], o_recv.at[r],
            device_id=sibling, device_id_type=MESH,
        )

    w_in[2].wait()
    w_far[2].wait_recv()
    sent_halo(0)
    for rows in inner:
        y = conv(2, rows, 0, ch)
        for i, r in enumerate(rows):
            act[0, r + 1, 1 : width + 1, :, half:ch] = y[i, :, :, half:ch]
            own[r] = y[i, :, :, 0:half]
        for r in rows:
            to_sibling(r).start()
    wait_halo(2)
    y = conv(2, outer, half, ch)
    for i, r in enumerate(outer):
        act[0, r + 1, 1 : width + 1, :, half:ch] = y[i]
    for r in outer:
        to_sibling(r).start()
    y = conv(2, outer, 0, half)
    for i, r in enumerate(outer):
        own[r] = y[i]

    for i in range(3):
        w_far[i].wait_send()
    for level in (1, 2):
        sent_halo(level)
    for c in b_far:
        c.wait_send()
    for r in range(height):
        to_sibling(r).wait_send()
        to_sibling(r).wait_recv()


def write(dims, own, far, out, stage, sem):
    per_core, height, width, half = dims
    core = lax.axis_index("model")

    def put(k, col):
        image = jnp.where(k == 0, core, 1 - core) * per_core
        return pltpu.make_async_copy(stage.at[k, :, col], out.at[pl.ds(image, per_core), col], sem.at[k, col])

    def column(col, _):
        for k, part in enumerate((own, far)):
            stage[k, :, col] = jnp.swapaxes(part[:, col], 0, 1)
            put(k, col).start()
        return 0

    lax.fori_loop(0, width, column, 0)

    def finish(col, _):
        for k in range(2):
            put(k, col).wait()
        return 0

    lax.fori_loop(0, width, finish, 0)


def solution(mesh):
    n_band = mesh.shape["spatial"]

    def local_stack(images, w_conv1, b_conv1, w_conv2, b_conv2, w_conv3, b_conv3):
        batch, height, width, ch = images.shape
        half, per_core = ch // 2, batch // 2
        hbm = pl.BlockSpec(memory_space=pltpu.HBM)
        vmem = pl.BlockSpec(memory_space=pltpu.VMEM)
        dma = pltpu.SemaphoreType.DMA
        part = (height, width, per_core, half)
        args = (
            jnp.swapaxes(images, 1, 2),
            w_conv1.reshape(9, ch, half), b_conv1.reshape(1, half),
            w_conv2.reshape(9, half, ch), b_conv2.reshape(1, ch),
            w_conv3.reshape(9, ch, half), b_conv3.reshape(1, half),
        )
        own, far = pl.pallas_call(
            functools.partial(convs, (n_band, per_core, height, width, ch)),
            out_shape=[pltpu.VMEM(part, jnp.bfloat16)] * 2,
            in_specs=[hbm] * 7,
            out_specs=[vmem] * 2,
            scratch_shapes=[
                pltpu.VMEM((per_core, width, height, ch), jnp.bfloat16),
                pltpu.VMEM((3, height + 2, width + 2, per_core, ch), jnp.bfloat16),
                pltpu.VMEM((3, 9, ch, ch), jnp.bfloat16),
                pltpu.VMEM((3, 1, half), jnp.float32),
                pltpu.VMEM((3, 1, half), jnp.float32),
                dma((width,)),
                dma((3,)), dma((3,)), dma((3,)),
                dma((4,)), dma((2,)), dma((2,)),
                dma((3, 2)), dma((3, 2)),
                dma((height,)), dma((height,)),
            ],
            compiler_params=pltpu.CompilerParams(
                collective_id=0, has_side_effects=True, vmem_limit_bytes=VMEM_LIMIT
            ),
            cost_estimate=pl.CostEstimate(
                flops=2 * 3 * 9 * per_core * height * width * ch * ch, bytes_accessed=20_000_000, transcendentals=0
            ),
        )(*[pltpu.with_memory_space_constraint(a, pltpu.HBM) for a in args])
        y = pl.pallas_call(
            functools.partial(write, (per_core, height, width, half)),
            out_shape=jax.ShapeDtypeStruct((batch, width, height, half), jnp.bfloat16),
            in_specs=[vmem] * 2,
            out_specs=hbm,
            scratch_shapes=[pltpu.VMEM((2, per_core, width, height, half), jnp.bfloat16), dma((2, width))],
            compiler_params=pltpu.CompilerParams(vmem_limit_bytes=16 * 1024 * 1024),
        )(own, far)
        return jnp.swapaxes(y, 1, 2)

    in_specs = (
        P("data", "spatial", None, None),
        P(None, None, None, "model"),
        P("model"),
        P(None, None, "model", None),
        P(None),
        P(None, None, None, "model"),
        P("model"),
    )
    return jax.shard_map(local_stack, mesh=mesh, in_specs=in_specs, out_specs=P("data", "spatial", None, "model"), check_vma=False)
```

```python
import functools

import jax
import jax.numpy as jnp
from jax import lax
from jax.experimental import pallas as pl
from jax.experimental.pallas import tpu as pltpu
from jax.sharding import PartitionSpec as P

MESH = pl.DeviceIdType.MESH
ROWS = 4
LINE = 4
VMEM_LIMIT = 48 * 1024 * 1024


def convs(
    dims, img, w1, b1, w2, b2, w3, b3, own, far,
    stage, act, wts, bias_own, bias_far,
    img_sem, w_sem, w_send, w_recv, b_sem, b_send, b_recv, h_send, h_recv, o_send, o_recv,
):
    n_band, per_core, height, width, ch = dims
    half = ch // 2
    core = lax.axis_index("model")
    band = lax.axis_index("spatial")
    data = lax.axis_index("data")
    first, final = band == 0, band == n_band - 1
    above, below = jnp.maximum(band - 1, 0), jnp.minimum(band + 1, n_band - 1)
    sibling = (data, band, 1 - core)

    def image_in(col):
        return pltpu.make_async_copy(img.at[pl.ds(core * per_core, per_core), col], stage.at[:, col], img_sem.at[col])

    own_parts = [wts.at[0, :, :, 0:half], wts.at[1, :, 0:half, :], wts.at[2, :, :, 0:half]]
    far_parts = [wts.at[0, :, :, half:ch], wts.at[1, :, half:ch, :], wts.at[2, :, :, half:ch]]
    w_in = [pltpu.make_async_copy(w, own_parts[i], w_sem.at[i]) for i, w in enumerate((w1, w2, w3))]
    w_far = [
        pltpu.make_async_remote_copy(w, far_parts[i], w_send.at[i], w_recv.at[i], device_id=sibling, device_id_type=MESH)
        for i, w in enumerate((w1, w2, w3))
    ]
    b_in = [
        pltpu.make_async_copy(b1, bias_own.at[0], b_sem.at[0]),
        pltpu.make_async_copy(b2.at[:, 0:half], bias_own.at[1], b_sem.at[1]),
        pltpu.make_async_copy(b2.at[:, half:ch], bias_far.at[1], b_sem.at[2]),
        pltpu.make_async_copy(b3, bias_own.at[2], b_sem.at[3]),
    ]
    b_far = [
        pltpu.make_async_remote_copy(b, bias_far.at[i], b_send.at[k], b_recv.at[k], device_id=sibling, device_id_type=MESH)
        for k, (b, i) in enumerate(((b1, 0), (b3, 2)))
    ]

    barrier = pltpu.get_barrier_semaphore()
    pl.semaphore_signal(barrier, inc=1, device_id=sibling, device_id_type=MESH)

    @pl.when(jnp.logical_not(first))
    def _():
        pl.semaphore_signal(barrier, inc=1, device_id=(data, above, core), device_id_type=MESH)

    @pl.when(jnp.logical_not(final))
    def _():
        pl.semaphore_signal(barrier, inc=1, device_id=(data, below, core), device_id_type=MESH)

    for col in range(width):
        image_in(col).start()
    w_in[0].start()
    for c in b_in:
        c.start()
    pl.semaphore_wait(barrier, 3 - first.astype(jnp.int32) - final.astype(jnp.int32))
    w_far[0].start()
    for c in b_far:
        c.start()

    zero_row = jnp.zeros((width, per_core, ch), jnp.bfloat16)
    zero_col = jnp.zeros((1, per_core, ch), jnp.bfloat16)

    def zero(level, _):
        def cols(r, _):
            act[level, r, 0:1] = zero_col
            act[level, r, width + 1 : width + 2] = zero_col
            return 0

        lax.fori_loop(0, height + 2, cols, 0)

        @pl.when(first)
        def _():
            act[level, 0, 1 : width + 1] = zero_row

        @pl.when(final)
        def _():
            act[level, height + 1, 1 : width + 1] = zero_row

        return 0

    lax.fori_loop(0, 3, zero, 0)

    def halo_up(level):
        return pltpu.make_async_remote_copy(
            act.at[level, 1, 1 : width + 1], act.at[level, height + 1, 1 : width + 1],
            h_send.at[level, 0], h_recv.at[level, 0], device_id=(data, above, core), device_id_type=MESH,
        )

    def halo_down(level):
        return pltpu.make_async_remote_copy(
            act.at[level, height, 1 : width + 1], act.at[level, 0, 1 : width + 1],
            h_send.at[level, 1], h_recv.at[level, 1], device_id=(data, below, core), device_id_type=MESH,
        )

    line_end = lax.rem(band, LINE) == LINE - 1

    def send_halo(level):
        @pl.when(jnp.logical_and(line_end, jnp.logical_not(final)))
        def _():
            halo_down(level).start()

        @pl.when(jnp.logical_not(first))
        def _():
            halo_up(level).start()

        @pl.when(jnp.logical_not(jnp.logical_or(line_end, final)))
        def _():
            halo_down(level).start()

    def wait_halo(level):
        @pl.when(jnp.logical_not(final))
        def _():
            halo_up(level).wait_recv()

        @pl.when(jnp.logical_not(first))
        def _():
            halo_down(level).wait_recv()

    def sent_halo(level):
        @pl.when(jnp.logical_not(first))
        def _():
            halo_up(level).wait_send()

        @pl.when(jnp.logical_not(final))
        def _():
            halo_down(level).wait_send()

    def take(col, _):
        image_in(col).wait()
        act[0, 1 : height + 1, col + 1] = jnp.swapaxes(stage[:, col], 0, 1)
        return 0

    lax.fori_loop(0, width, take, 0)
    send_halo(0)
    w_in[1].start()
    w_in[2].start()
    w_far[1].start()
    w_far[2].start()

    def conv(level, rows, lo, hi):
        m = width * per_core
        taps = []
        for dh in range(3):
            for dw in range(3):
                views = [act[level, r + dh, dw : dw + width].reshape(m, ch) for r in rows]
                taps.append(jnp.concatenate(views, axis=0))
        lhs = jnp.concatenate(taps, axis=1)
        total = jnp.dot(lhs, wts[level, :, :, lo:hi].reshape(9 * ch, hi - lo), preferred_element_type=jnp.float32)
        bias = ([bias_own[level]] if lo == 0 else []) + ([bias_far[level]] if hi == ch else [])
        total = total + (jnp.concatenate(bias, axis=1) if len(bias) > 1 else bias[0])
        return jnp.maximum(total, 0.0).astype(jnp.bfloat16).reshape(len(rows), width, per_core, hi - lo)

    def step(level, rows, lo=0, hi=ch):
        y = conv(level, rows, lo, hi)
        for i, r in enumerate(rows):
            act[level + 1, r + 1, 1 : width + 1, :, lo:hi] = y[i]

    inner = [list(range(r, min(r + ROWS, height - 1))) for r in range(1, height - 1, ROWS)]
    outer = [height - 1, 0]

    w_in[0].wait()
    for c in b_in:
        c.wait()
    for rows in inner[:2]:
        step(0, rows, 0, half)
    w_far[0].wait_recv()
    for c in b_far:
        c.wait_recv()
    for rows in inner[:2]:
        step(0, rows, half, ch)
    for rows in inner[2:]:
        step(0, rows)
    wait_halo(0)
    step(0, outer)
    send_halo(1)

    w_in[1].wait()
    w_far[1].wait_recv()
    for rows in inner:
        step(1, rows)
    wait_halo(1)
    step(1, outer)
    send_halo(2)

    def to_sibling(r):
        return pltpu.make_async_remote_copy(
            act.at[0, r + 1, 1 : width + 1, :, half:ch], far.at[r], o_send.at[r], o_recv.at[r],
            device_id=sibling, device_id_type=MESH,
        )

    w_in[2].wait()
    w_far[2].wait_recv()
    sent_halo(0)
    def last(rows, lo, hi):
        y = conv(2, rows, lo, hi)
        for i, r in enumerate(rows):
            if lo == 0:
                own[r] = y[i, :, :, 0:half]
            if hi == ch:
                act[0, r + 1, 1 : width + 1, :, half:ch] = y[i, :, :, half - lo : ch - lo]

    def send(groups):
        for rows in groups:
            for r in rows:
                to_sibling(r).start()

    for rows in inner[:2]:
        last(rows, 0, ch)
    send(inner[:2])
    for rows in inner[2:]:
        last(rows, 0, ch)
    send(inner[2:])
    wait_halo(2)
    for r in outer:
        last([r], half, ch)
    send([outer])
    for r in outer:
        last([r], 0, half)

    for i in range(3):
        w_far[i].wait_send()
    for level in (1, 2):
        sent_halo(level)
    for c in b_far:
        c.wait_send()
    for r in range(height):
        to_sibling(r).wait_send()
        to_sibling(r).wait_recv()


def write(dims, own, far, out, stage, sem):
    per_core, height, width, half = dims
    core = lax.axis_index("model")

    def put(k, col):
        image = jnp.where(k == 0, core, 1 - core) * per_core
        return pltpu.make_async_copy(stage.at[k, :, col], out.at[pl.ds(image, per_core), col], sem.at[k, col])

    def column(col, _):
        for k, part in enumerate((own, far)):
            stage[k, :, col] = jnp.swapaxes(part[:, col], 0, 1)
            put(k, col).start()
        return 0

    lax.fori_loop(0, width, column, 0)

    def finish(col, _):
        for k in range(2):
            put(k, col).wait()
        return 0

    lax.fori_loop(0, width, finish, 0)


def solution(mesh):
    n_band = mesh.shape["spatial"]

    def local_stack(images, w_conv1, b_conv1, w_conv2, b_conv2, w_conv3, b_conv3):
        batch, height, width, ch = images.shape
        half, per_core = ch // 2, batch // 2
        hbm = pl.BlockSpec(memory_space=pltpu.HBM)
        vmem = pl.BlockSpec(memory_space=pltpu.VMEM)
        dma = pltpu.SemaphoreType.DMA
        part = (height, width, per_core, half)
        args = (
            jnp.swapaxes(images, 1, 2),
            w_conv1.reshape(9, ch, half), b_conv1.reshape(1, half),
            w_conv2.reshape(9, half, ch), b_conv2.reshape(1, ch),
            w_conv3.reshape(9, ch, half), b_conv3.reshape(1, half),
        )
        own, far = pl.pallas_call(
            functools.partial(convs, (n_band, per_core, height, width, ch)),
            out_shape=[pltpu.VMEM(part, jnp.bfloat16)] * 2,
            in_specs=[hbm] * 7,
            out_specs=[vmem] * 2,
            scratch_shapes=[
                pltpu.VMEM((per_core, width, height, ch), jnp.bfloat16),
                pltpu.VMEM((3, height + 2, width + 2, per_core, ch), jnp.bfloat16),
                pltpu.VMEM((3, 9, ch, ch), jnp.bfloat16),
                pltpu.VMEM((3, 1, half), jnp.float32),
                pltpu.VMEM((3, 1, half), jnp.float32),
                dma((width,)),
                dma((3,)), dma((3,)), dma((3,)),
                dma((4,)), dma((2,)), dma((2,)),
                dma((3, 2)), dma((3, 2)),
                dma((height,)), dma((height,)),
            ],
            compiler_params=pltpu.CompilerParams(
                collective_id=0, has_side_effects=True, vmem_limit_bytes=VMEM_LIMIT
            ),
            cost_estimate=pl.CostEstimate(
                flops=2 * 3 * 9 * per_core * height * width * ch * ch, bytes_accessed=20_000_000, transcendentals=0
            ),
        )(*[pltpu.with_memory_space_constraint(a, pltpu.HBM) for a in args])
        y = pl.pallas_call(
            functools.partial(write, (per_core, height, width, half)),
            out_shape=jax.ShapeDtypeStruct((batch, width, height, half), jnp.bfloat16),
            in_specs=[vmem] * 2,
            out_specs=hbm,
            scratch_shapes=[pltpu.VMEM((2, per_core, width, height, half), jnp.bfloat16), dma((2, width))],
            compiler_params=pltpu.CompilerParams(vmem_limit_bytes=16 * 1024 * 1024),
        )(own, far)
        return jnp.swapaxes(y, 1, 2)

    in_specs = (
        P("data", "spatial", None, None),
        P(None, None, None, "model"),
        P("model"),
        P(None, None, "model", None),
        P(None),
        P(None, None, None, "model"),
        P("model"),
    )
    return jax.shard_map(local_stack, mesh=mesh, in_specs=in_specs, out_specs=P("data", "spatial", None, "model"), check_vma=False)
```

```python
import functools

import jax
import jax.numpy as jnp
from jax import lax
from jax.experimental import pallas as pl
from jax.experimental.pallas import tpu as pltpu
from jax.sharding import PartitionSpec as P

MESH = pl.DeviceIdType.MESH
ROWS = 4
LINE = 4
VMEM_LIMIT = 48 * 1024 * 1024


def convs(
    dims, img, w1, b1, w2, b2, w3, b3, own, far,
    stage, act, wts, bias_own, bias_far,
    img_sem, w_sem, w_send, w_recv, b_sem, b_send, b_recv, h_send, h_recv, o_send, o_recv,
):
    n_band, per_core, height, width, ch = dims
    half = ch // 2
    core = lax.axis_index("model")
    band = lax.axis_index("spatial")
    data = lax.axis_index("data")
    first, final = band == 0, band == n_band - 1
    above, below = jnp.maximum(band - 1, 0), jnp.minimum(band + 1, n_band - 1)
    sibling = (data, band, 1 - core)

    def image_in(col):
        return pltpu.make_async_copy(img.at[pl.ds(core * per_core, per_core), col], stage.at[:, col], img_sem.at[col])

    own_parts = [wts.at[0, :, :, 0:half], wts.at[1, :, 0:half, :], wts.at[2, :, :, 0:half]]
    far_parts = [wts.at[0, :, :, half:ch], wts.at[1, :, half:ch, :], wts.at[2, :, :, half:ch]]
    w_in = [pltpu.make_async_copy(w, own_parts[i], w_sem.at[i]) for i, w in enumerate((w1, w2, w3))]
    w_far = [
        pltpu.make_async_remote_copy(w, far_parts[i], w_send.at[i], w_recv.at[i], device_id=sibling, device_id_type=MESH)
        for i, w in enumerate((w1, w2, w3))
    ]
    b_in = [
        pltpu.make_async_copy(b1, bias_own.at[0], b_sem.at[0]),
        pltpu.make_async_copy(b2.at[:, 0:half], bias_own.at[1], b_sem.at[1]),
        pltpu.make_async_copy(b2.at[:, half:ch], bias_far.at[1], b_sem.at[2]),
        pltpu.make_async_copy(b3, bias_own.at[2], b_sem.at[3]),
    ]
    b_far = [
        pltpu.make_async_remote_copy(b, bias_far.at[i], b_send.at[k], b_recv.at[k], device_id=sibling, device_id_type=MESH)
        for k, (b, i) in enumerate(((b1, 0), (b3, 2)))
    ]

    barrier = pltpu.get_barrier_semaphore()
    pl.semaphore_signal(barrier, inc=1, device_id=sibling, device_id_type=MESH)

    @pl.when(jnp.logical_not(first))
    def _():
        pl.semaphore_signal(barrier, inc=1, device_id=(data, above, core), device_id_type=MESH)

    @pl.when(jnp.logical_not(final))
    def _():
        pl.semaphore_signal(barrier, inc=1, device_id=(data, below, core), device_id_type=MESH)

    for col in range(width):
        image_in(col).start()
    w_in[0].start()
    for c in b_in:
        c.start()

    zero_row = jnp.zeros((width, per_core, ch), jnp.bfloat16)
    zero_col = jnp.zeros((1, per_core, ch), jnp.bfloat16)

    def zero(level, _):
        def cols(r, _):
            act[level, r, 0:1] = zero_col
            act[level, r, width + 1 : width + 2] = zero_col
            return 0

        lax.fori_loop(0, height + 2, cols, 0)

        @pl.when(first)
        def _():
            act[level, 0, 1 : width + 1] = zero_row

        @pl.when(final)
        def _():
            act[level, height + 1, 1 : width + 1] = zero_row

        return 0

    lax.fori_loop(0, 3, zero, 0)

    def halo_up(level):
        return pltpu.make_async_remote_copy(
            act.at[level, 1, 1 : width + 1], act.at[level, height + 1, 1 : width + 1],
            h_send.at[level, 0], h_recv.at[level, 0], device_id=(data, above, core), device_id_type=MESH,
        )

    def halo_down(level):
        return pltpu.make_async_remote_copy(
            act.at[level, height, 1 : width + 1], act.at[level, 0, 1 : width + 1],
            h_send.at[level, 1], h_recv.at[level, 1], device_id=(data, below, core), device_id_type=MESH,
        )

    line_end = lax.rem(band, LINE) == LINE - 1

    def send_halo(level):
        @pl.when(jnp.logical_and(line_end, jnp.logical_not(final)))
        def _():
            halo_down(level).start()

        @pl.when(jnp.logical_not(first))
        def _():
            halo_up(level).start()

        @pl.when(jnp.logical_not(jnp.logical_or(line_end, final)))
        def _():
            halo_down(level).start()

    def wait_halo(level):
        @pl.when(jnp.logical_not(final))
        def _():
            halo_up(level).wait_recv()

        @pl.when(jnp.logical_not(first))
        def _():
            halo_down(level).wait_recv()

    def sent_halo(level):
        @pl.when(jnp.logical_not(first))
        def _():
            halo_up(level).wait_send()

        @pl.when(jnp.logical_not(final))
        def _():
            halo_down(level).wait_send()

    def take(col, _):
        image_in(col).wait()
        act[0, 1 : height + 1, col + 1] = jnp.swapaxes(stage[:, col], 0, 1)
        return 0

    lax.fori_loop(0, width, take, 0)
    w_in[1].start()
    w_in[2].start()

    def conv(level, rows, lo, hi):
        m = width * per_core
        taps = []
        for dh in range(3):
            for dw in range(3):
                views = [act[level, r + dh, dw : dw + width].reshape(m, ch) for r in rows]
                taps.append(jnp.concatenate(views, axis=0))
        lhs = jnp.concatenate(taps, axis=1)
        total = jnp.dot(lhs, wts[level, :, :, lo:hi].reshape(9 * ch, hi - lo), preferred_element_type=jnp.float32)
        bias = ([bias_own[level]] if lo == 0 else []) + ([bias_far[level]] if hi == ch else [])
        total = total + (jnp.concatenate(bias, axis=1) if len(bias) > 1 else bias[0])
        return jnp.maximum(total, 0.0).astype(jnp.bfloat16).reshape(len(rows), width, per_core, hi - lo)

    def step(level, rows, lo=0, hi=ch):
        y = conv(level, rows, lo, hi)
        for i, r in enumerate(rows):
            act[level + 1, r + 1, 1 : width + 1, :, lo:hi] = y[i]

    inner = [list(range(r, min(r + ROWS, height - 1))) for r in range(1, height - 1, ROWS)]
    outer = [height - 1, 0]

    w_in[0].wait()
    for c in b_in:
        c.wait()
    step(0, [1, 2], 0, half)
    step(0, [3, 4], 0, half)
    pl.semaphore_wait(barrier, 3 - first.astype(jnp.int32) - final.astype(jnp.int32))
    w_far[0].start()
    for c in b_far:
        c.start()
    send_halo(0)
    w_far[1].start()
    w_far[2].start()
    rest = list(range(5, height - 1))
    pairs = [rest[:4], rest[4:8]] + [[r] for r in rest[8:]]
    for rows in pairs:
        step(0, rows, 0, half)
    w_far[0].wait_recv()
    for c in b_far:
        c.wait_recv()
    for rows in ([1, 2, 3, 4], rest[:4], rest[4:7], rest[7:]):
        step(0, rows, half, ch)
    wait_halo(0)
    step(0, outer)
    send_halo(1)

    w_in[1].wait()
    w_far[1].wait_recv()
    for rows in inner:
        step(1, rows)
    wait_halo(1)
    step(1, outer)
    send_halo(2)

    def to_sibling(r):
        return pltpu.make_async_remote_copy(
            act.at[0, r + 1, 1 : width + 1, :, half:ch], far.at[r], o_send.at[r], o_recv.at[r],
            device_id=sibling, device_id_type=MESH,
        )

    w_in[2].wait()
    w_far[2].wait_recv()
    sent_halo(0)
    def last(rows, lo, hi):
        y = conv(2, rows, lo, hi)
        for i, r in enumerate(rows):
            if lo == 0:
                own[r] = y[i, :, :, 0:half]
            if hi == ch:
                act[0, r + 1, 1 : width + 1, :, half:ch] = y[i, :, :, half - lo : ch - lo]

    def send(groups):
        for rows in groups:
            for r in rows:
                to_sibling(r).start()

    for rows in inner[:2]:
        last(rows, 0, ch)
    send(inner[:2])
    for rows in inner[2:]:
        last(rows, 0, ch)
    send(inner[2:])
    wait_halo(2)
    for r in outer:
        last([r], half, ch)
    send([outer])
    for r in outer:
        last([r], 0, half)

    for i in range(3):
        w_far[i].wait_send()
    for level in (1, 2):
        sent_halo(level)
    for c in b_far:
        c.wait_send()
    for r in range(height):
        to_sibling(r).wait_send()
        to_sibling(r).wait_recv()


def write(dims, own, far, out, stage, sem):
    per_core, height, width, half = dims
    core = lax.axis_index("model")

    def put(k, col):
        image = jnp.where(k == 0, core, 1 - core) * per_core
        return pltpu.make_async_copy(stage.at[k, :, col], out.at[pl.ds(image, per_core), col], sem.at[k, col])

    def column(col, _):
        for k, part in enumerate((own, far)):
            stage[k, :, col] = jnp.swapaxes(part[:, col], 0, 1)
            put(k, col).start()
        return 0

    lax.fori_loop(0, width, column, 0)

    def finish(col, _):
        for k in range(2):
            put(k, col).wait()
        return 0

    lax.fori_loop(0, width, finish, 0)


def solution(mesh):
    n_band = mesh.shape["spatial"]

    def local_stack(images, w_conv1, b_conv1, w_conv2, b_conv2, w_conv3, b_conv3):
        batch, height, width, ch = images.shape
        half, per_core = ch // 2, batch // 2
        hbm = pl.BlockSpec(memory_space=pltpu.HBM)
        vmem = pl.BlockSpec(memory_space=pltpu.VMEM)
        dma = pltpu.SemaphoreType.DMA
        part = (height, width, per_core, half)
        args = (
            jnp.swapaxes(images, 1, 2),
            w_conv1.reshape(9, ch, half), b_conv1.reshape(1, half),
            w_conv2.reshape(9, half, ch), b_conv2.reshape(1, ch),
            w_conv3.reshape(9, ch, half), b_conv3.reshape(1, half),
        )
        own, far = pl.pallas_call(
            functools.partial(convs, (n_band, per_core, height, width, ch)),
            out_shape=[pltpu.VMEM(part, jnp.bfloat16)] * 2,
            in_specs=[hbm] * 7,
            out_specs=[vmem] * 2,
            scratch_shapes=[
                pltpu.VMEM((per_core, width, height, ch), jnp.bfloat16),
                pltpu.VMEM((3, height + 2, width + 2, per_core, ch), jnp.bfloat16),
                pltpu.VMEM((3, 9, ch, ch), jnp.bfloat16),
                pltpu.VMEM((3, 1, half), jnp.float32),
                pltpu.VMEM((3, 1, half), jnp.float32),
                dma((width,)),
                dma((3,)), dma((3,)), dma((3,)),
                dma((4,)), dma((2,)), dma((2,)),
                dma((3, 2)), dma((3, 2)),
                dma((height,)), dma((height,)),
            ],
            compiler_params=pltpu.CompilerParams(
                collective_id=0, has_side_effects=True, vmem_limit_bytes=VMEM_LIMIT
            ),
            cost_estimate=pl.CostEstimate(
                flops=2 * 3 * 9 * per_core * height * width * ch * ch, bytes_accessed=20_000_000, transcendentals=0
            ),
        )(*[pltpu.with_memory_space_constraint(a, pltpu.HBM) for a in args])
        y = pl.pallas_call(
            functools.partial(write, (per_core, height, width, half)),
            out_shape=jax.ShapeDtypeStruct((batch, width, height, half), jnp.bfloat16),
            in_specs=[vmem] * 2,
            out_specs=hbm,
            scratch_shapes=[pltpu.VMEM((2, per_core, width, height, half), jnp.bfloat16), dma((2, width))],
            compiler_params=pltpu.CompilerParams(vmem_limit_bytes=16 * 1024 * 1024),
        )(own, far)
        return jnp.swapaxes(y, 1, 2)

    in_specs = (
        P("data", "spatial", None, None),
        P(None, None, None, "model"),
        P("model"),
        P(None, None, "model", None),
        P(None),
        P(None, None, None, "model"),
        P("model"),
    )
    return jax.shard_map(local_stack, mesh=mesh, in_specs=in_specs, out_specs=P("data", "spatial", None, "model"), check_vma=False)
```
